32 devices in a mesh: dp: 1 (over z), tp: 4 (over y), fsdp: 8 (over x, core).
Axes of the slice: x: 4, y: 4, z: 1, core: 2. Of those that a mesh axis runs over, the one named last changes fastest.
The devices are a block of a 4x4x8 slice.
Arguments:
- tokens: int32 [128, 2048], P(('dp', 'fsdp'))
- out_grad: bfloat16 [128, 2048, 1024], P(('dp', 'fsdp'))
- head_grad: float32 [32128, 1024], P(('dp', 'tp'), 'fsdp')
- master_w: float32 [32128, 1024], P(('dp', 'tp'), 'fsdp')
- moment_m: float32 [32128, 1024], P(('dp', 'tp'), 'fsdp')
- moment_v: float32 [32128, 1024], P(('dp', 'tp'), 'fsdp')
- learn_rate: float32 [], replicated
- clip_scale: float32 [], replicated
Outputs:
- output 1: float32 [32128, 1024], P(('dp', 'tp'), 'fsdp')
- output 2: float32 [32128, 1024], P(('dp', 'tp'), 'fsdp')
- output 3: float32 [32128, 1024], P(('dp', 'tp'), 'fsdp')
- output 4: bfloat16 [32128, 1024], P(('dp', 'tp'), 'fsdp')
All inputs are finite; a program needn't handle non-finite values.
Results may differ from the reference program's by a relative error of at most 0.001.
Values sent between devices are 32-bit elements.
A program may use at most 768 MiB of HBM per device.

```python
import math
import jax
import jax.numpy as jnp

VOCAB_SIZE = 32128
MODEL_DIM = 1024
BATCH_ROWS = 128
SEQ_LEN = 2048
OPT_STEP = 20
TOKEN_LEVELS = int(math.ceil(math.log2(VOCAB_SIZE)))


def draw_tokens(tok_key):
    level_key, value_key, shift_key = jax.random.split(tok_key, 3)
    tok_shape = (BATCH_ROWS, SEQ_LEN)
    levels = jax.random.randint(level_key, tok_shape, 0, TOKEN_LEVELS + 1, dtype=jnp.int32)
    widths = jnp.minimum(jnp.left_shift(jnp.int32(1), levels), VOCAB_SIZE)
    raw_ids = jax.random.randint(value_key, tok_shape, 0, 2 ** 30, dtype=jnp.int32) % widths
    token_shift = jax.random.randint(shift_key, (), 0, VOCAB_SIZE, dtype=jnp.int32)
    tokens = (raw_ids + token_shift) % VOCAB_SIZE
    return tokens.at[0, 0].set(0).at[0, 1].set(VOCAB_SIZE - 1)


def setup_inputs(seed: int = 0, part: int = 0) -> dict:
    base_key = jax.random.key(seed)
    part_key = jax.random.fold_in(base_key, part)
    tok_key, grad_key, head_key, emb_key, mom_key, vel_key = jax.random.split(part_key, 6)
    lr_key, clip_key = jax.random.split(base_key, 2)
    table_shape = (VOCAB_SIZE, MODEL_DIM)
    tokens = draw_tokens(tok_key)
    out_grad = jax.random.normal(grad_key, (BATCH_ROWS, SEQ_LEN, MODEL_DIM), jnp.float32).astype(jnp.bfloat16)
    head_grad = 0.25 * jax.random.normal(head_key, table_shape, jnp.float32)
    master_w = MODEL_DIM ** -0.5 * jax.random.normal(emb_key, table_shape, jnp.float32)
    moment_m = 0.3 * jax.random.normal(mom_key, table_shape, jnp.float32)
    moment_v = 0.0625 * (0.5 + jax.random.uniform(vel_key, table_shape, jnp.float32))
    learn_rate = 0.01 + 0.04 * jax.random.uniform(lr_key, (), jnp.float32)
    clip_scale = 0.5 + 0.5 * jax.random.uniform(clip_key, (), jnp.float32)
    return {"tokens": tokens, "out_grad": out_grad, "head_grad": head_grad, "master_w": master_w, "moment_m": moment_m, "moment_v": moment_v, "learn_rate": learn_rate, "clip_scale": clip_scale}


def reference(tokens, out_grad, head_grad, master_w, moment_m, moment_v, learn_rate, clip_scale):
    beta_two = 1.0 - OPT_STEP ** -0.8
    flat_rows = out_grad.reshape(-1, MODEL_DIM).astype(jnp.float32)
    embed_grad = jax.ops.segment_sum(flat_rows, tokens.reshape(-1), num_segments=VOCAB_SIZE)
    grad_full = clip_scale * (embed_grad + head_grad)
    new_v = beta_two * moment_v + (1.0 - beta_two) * (grad_full * grad_full + 1e-30)
    update = grad_full / jnp.sqrt(new_v)
    new_m = 0.9 * moment_m + 0.1 * update
    new_w = master_w - learn_rate * new_m - learn_rate * learn_rate * master_w
    return (new_w, new_m, new_v, new_w.astype(jnp.bfloat16))
```

```python
import functools

import jax
import jax.numpy as jnp
from jax import lax
from jax.experimental import pallas as pl
from jax.experimental.pallas import tpu as pltpu
from jax.sharding import PartitionSpec as P

OPT_STEP = 20
LANES = 128
TILE = 256
GROUP = 16
CORES = 2
PIECES = 8
MESH = pl.DeviceIdType.MESH


def adafactor_update(embed_grad, head_grad, master_w, moment_m, moment_v, learn_rate, clip_scale):
    beta_two = 1.0 - OPT_STEP ** -0.8
    grad_full = clip_scale * (embed_grad + head_grad)
    new_v = beta_two * moment_v + (1.0 - beta_two) * (grad_full * grad_full + 1e-30)
    new_m = 0.9 * moment_m + 0.1 * (grad_full / jnp.sqrt(new_v))
    new_w = master_w - learn_rate * new_m - learn_rate * learn_rate * master_w
    return new_w, new_m, new_v, new_w.astype(jnp.bfloat16)


def unique_lists(tokens, n_class, rows):
    n_seq, seq_len = tokens.shape
    bits = int(rows).bit_length()
    me = lax.axis_index("tp")
    mine = tokens % n_class == me
    seq = lax.broadcasted_iota(jnp.int32, tokens.shape, 0)
    high = seq << (bits + 1)
    flag = 1 << bits
    key = jnp.where(mine, high + tokens // n_class, high + flag).reshape(-1)
    key = lax.sort(key)
    previous = jnp.concatenate([jnp.full((1,), -1, key.dtype), key[:-1]])
    padding = (key >> (bits + 1) << (bits + 1)) + flag
    key = lax.sort(jnp.where(key == previous, padding, key))
    slots = (key & (2 * flag - 1)).reshape(n_seq, seq_len)
    valid = slots < flag
    counts = jnp.sum(valid.astype(jnp.int32), axis=1)
    full = jnp.where(valid, slots * n_class + me, -1)
    return jnp.where(valid, slots, rows), full, counts


def scatter_kernel(rows, pitch, slot_ref, count_ref, tok_ref, full_ref, x_ref, out_ref, acc, onehot, sums, sem):
    b = pl.program_id(0)
    blocks = x_ref.shape[2] // LANES
    seq_len = x_ref.shape[1]
    sum_pitch = sums.shape[0] // blocks

    @pl.when(b == 0)
    def _():
        step = 8 * 67 if acc.shape[0] % (8 * 67) == 0 else 8

        def zero(i, carry):
            acc[pl.ds(pl.multiple_of(i * step, 8), step), :] = jnp.zeros((step, LANES), jnp.float32)
            return carry

        lax.fori_loop(0, acc.shape[0] // step, zero, 0)

    count = count_ref[b]
    tok = tok_ref[0]

    def tile(k, carry):
        row = full_ref[0, pl.ds(k, 1), :]
        eye = lax.broadcasted_iota(jnp.int32, (TILE, TILE), 0) == lax.broadcasted_iota(jnp.int32, (TILE, TILE), 1)
        col = jnp.sum(jnp.where(eye, row.astype(jnp.float32), 0.0), axis=1, keepdims=True).astype(jnp.int32)
        chunk = 512
        for j in range(0, seq_len, chunk):
            hit = col == tok[:, j : j + chunk]
            onehot[:, j : j + chunk] = jnp.where(hit, 1.0, 0.0).astype(jnp.bfloat16)
        for c in range(0, blocks, 2):
            part = jnp.dot(onehot[...], x_ref[0, :, c * LANES : (c + 2) * LANES], preferred_element_type=jnp.float32)
            sums[c * sum_pitch : c * sum_pitch + TILE, :] = part[:, :LANES]
            sums[(c + 1) * sum_pitch : (c + 1) * sum_pitch + TILE, :] = part[:, LANES:]

        left = jnp.minimum(count - k * TILE, TILE)

        def group(g, carry):
            base = b * seq_len + k * TILE + g * GROUP
            ids = [slot_ref[base + i] for i in range(GROUP)]
            old = [acc[pl.ds(v, blocks, stride=pitch), :] for v in ids]
            new = [a + sums[pl.ds(g * GROUP + i, blocks, stride=sum_pitch), :] for i, a in enumerate(old)]
            for v, a in zip(ids, new):
                acc[pl.ds(v, blocks, stride=pitch), :] = a
            return carry

        lax.fori_loop(0, (left + GROUP - 1) // GROUP, group, 0)
        return carry

    lax.fori_loop(0, (count + TILE - 1) // TILE, tile, 0)

    @pl.when(b == pl.num_programs(0) - 1)
    def _():
        copies = [
            pltpu.make_async_copy(acc.at[pl.ds(c * pitch, rows), :], out_ref.at[c], sem.at[c]) for c in range(blocks)
        ]
        for copy in copies:
            copy.start()
        for copy in copies:
            copy.wait()


def class_sums(tokens, out_grad, n_class, rows):
    n_seq, seq_len, width = out_grad.shape
    blocks = width // LANES
    pitch = rows + 8
    slots, full, counts = unique_lists(tokens, n_class, rows)
    return pl.pallas_call(
        functools.partial(scatter_kernel, rows, pitch),
        out_shape=jax.ShapeDtypeStruct((blocks, rows, LANES), jnp.float32),
        grid_spec=pltpu.PrefetchScalarGridSpec(
            num_scalar_prefetch=2,
            grid=(n_seq,),
            in_specs=[
                pl.BlockSpec((1, 1, seq_len), lambda b, *_: (b, 0, 0)),
                pl.BlockSpec((1, seq_len // TILE, TILE), lambda b, *_: (b, 0, 0)),
                pl.BlockSpec((1, seq_len, width), lambda b, *_: (b, 0, 0)),
            ],
            out_specs=pl.BlockSpec(memory_space=pl.ANY),
            scratch_shapes=[
                pltpu.VMEM((blocks * pitch, LANES), jnp.float32),
                pltpu.VMEM((TILE, seq_len), jnp.bfloat16),
                pltpu.VMEM((blocks * (TILE + 8), LANES), jnp.float32),
                pltpu.SemaphoreType.DMA((blocks,)),
            ],
        ),
        compiler_params=pltpu.CompilerParams(vmem_limit_bytes=60 * 1024 * 1024, dimension_semantics=("arbitrary",)),
        name="class_sums",
    )(slots.reshape(-1), counts, tokens.reshape(n_seq, 1, seq_len), full.reshape(n_seq, seq_len // TILE, TILE), out_grad)


def split_rows(rows, pieces):
    tiles = rows // 8
    sizes = [tiles // (2 * pieces) + (i < tiles % (2 * pieces)) for i in range(2 * pieces)]
    starts = [8 * sum(sizes[:i]) for i in range(2 * pieces)]
    spans = [(s, 8 * n) for s, n in zip(starts, sizes)]
    return spans[0::2], spans[1::2]


def exchange_kernel(n_x, n_tp, spans, part, out, own, sib, rec, got, load_sem, sib_sem, ring_sem, y_sem):
    pos = lax.axis_index("fsdp")
    me_y = lax.axis_index("tp")
    core = lax.rem(pos, CORES)
    me_x = pos // CORES
    other = 1 - core

    def at_x(x):
        return {"fsdp": lax.rem(x + n_x, n_x) * CORES + core}

    def at_y(d):
        return {"tp": lax.rem(me_y + d, n_tp)}

    sibling = {"fsdp": me_x * CORES + other}
    sides = [at_x(me_x + 1), at_x(me_x + n_x - 1)]

    barrier = pltpu.get_barrier_semaphore()
    peers = [sibling] + sides + [at_y(d) for d in range(1, n_tp)]
    for peer in peers:
        pl.semaphore_signal(barrier, inc=1, device_id=peer, device_id_type=MESH)
    pl.semaphore_wait(barrier, len(peers))

    def load(p, d):
        s, n = spans[d][p]
        return pltpu.make_async_copy(part.at[:, core, :, pl.ds(s, n), :], own.at[:, :, pl.ds(s, n), :], load_sem.at[d, p])

    def to_sibling(p, d):
        s, n = spans[d][p]
        return pltpu.make_async_remote_copy(
            src_ref=part.at[:, other, :, pl.ds(s, n), :],
            dst_ref=sib.at[:, :, pl.ds(s, n), :],
            send_sem=sib_sem.at[0, d, p],
            recv_sem=sib_sem.at[1, d, p],
            device_id=sibling,
            device_id_type=MESH,
        )

    def owner(d, step):
        return lax.rem(me_x + n_x - step, n_x) if d == 0 else lax.rem(me_x + step, n_x)

    def hop(p, d, step):
        s, n = spans[d][p]
        return pltpu.make_async_remote_copy(
            src_ref=own.at[owner(d, step), :, pl.ds(s, n), :],
            dst_ref=rec.at[step - 1, :, pl.ds(s, n), :],
            send_sem=ring_sem.at[0, d, step - 1, p],
            recv_sem=ring_sem.at[1, d, step - 1, p],
            device_id=sides[d],
            device_id_type=MESH,
        )

    def to_row(p, d, k):
        s, n = spans[d][p]
        return pltpu.make_async_remote_copy(
            src_ref=own.at[me_x, lax.rem(me_y + k, n_tp), pl.ds(s, n), :],
            dst_ref=got.at[k - 1, pl.ds(s, n), :],
            send_sem=y_sem.at[0, d, k - 1, p],
            recv_sem=y_sem.at[1, d, k - 1, p],
            device_id=at_y(k),
            device_id_type=MESH,
        )

    def add(p, d, step):
        s, n = spans[d][p]
        x = owner(d, step)
        for y in range(n_tp):
            total = own[x, y, pl.ds(s, n), :] + sib[x, y, pl.ds(s, n), :]
            if step > 1:
                total = total + rec[step - 2, y, pl.ds(s, n), :]
            own[x, y, pl.ds(s, n), :] = total

    pieces = len(spans[0])
    for p in range(pieces):
        for d in range(2):
            load(p, d).start()
            to_sibling(p, d).start()

    for t in range(pieces + n_x - 1):
        for step in range(1, n_x + 1):
            p = t - step + 1
            if not 0 <= p < pieces:
                continue
            for d in range(2):
                if step == 1:
                    load(p, d).wait()
                    to_sibling(p, d).wait_recv()
                else:
                    hop(p, d, step - 1).wait_recv()
                add(p, d, step)
                if step < n_x:
                    hop(p, d, step).start()
                else:
                    for k in range(1, n_tp):
                        to_row(p, d, k).start()

    for p in range(pieces):
        for d in range(2):
            s, n = spans[d][p]
            out[pl.ds(s * n_tp + me_y, n, stride=n_tp), :] = own[me_x, me_y, pl.ds(s, n), :]
            for k in range(1, n_tp):
                to_row(p, d, k).wait_recv()
                source = lax.rem(me_y + n_tp - k, n_tp)
                out[pl.ds(s * n_tp + source, n, stride=n_tp), :] = got[k - 1, pl.ds(s, n), :]

    for p in range(pieces):
        for d in range(2):
            to_sibling(p, d).wait_send()
            for step in range(1, n_x):
                hop(p, d, step).wait_send()
            for k in range(1, n_tp):
                to_row(p, d, k).wait_send()


def reduce_and_place(part, n_x, n_tp, rows):
    sub = rows // n_tp
    spans = split_rows(sub, PIECES)
    full = (n_x, n_tp, sub, LANES)
    return pl.pallas_call(
        functools.partial(exchange_kernel, n_x, n_tp, spans),
        out_shape=jax.ShapeDtypeStruct((rows, LANES), jnp.float32),
        in_specs=[pl.BlockSpec(memory_space=pl.ANY)],
        out_specs=pl.BlockSpec(memory_space=pltpu.VMEM),
        scratch_shapes=[
            pltpu.VMEM(full, jnp.float32),
            pltpu.VMEM(full, jnp.float32),
            pltpu.VMEM((n_x - 1, n_tp, sub, LANES), jnp.float32),
            pltpu.VMEM((n_tp - 1, sub, LANES), jnp.float32),
            pltpu.SemaphoreType.DMA((2, PIECES)),
            pltpu.SemaphoreType.DMA((2, 2, PIECES)),
            pltpu.SemaphoreType.DMA((2, 2, n_x - 1, PIECES)),
            pltpu.SemaphoreType.DMA((2, 2, n_tp - 1, PIECES)),
        ],
        compiler_params=pltpu.CompilerParams(
            collective_id=0, has_side_effects=True, vmem_limit_bytes=62 * 1024 * 1024
        ),
        name="reduce_and_place",
    )(part.reshape(n_x, CORES, n_tp, sub, LANES))


def solution(mesh):
    row_spec = P(("dp", "fsdp"), None)
    act_spec = P(("dp", "fsdp"), None, None)
    table_spec = P(("dp", "tp"), "fsdp")
    n_tp = mesh.shape["tp"]
    n_x = mesh.shape["fsdp"] // CORES

    def local_step(tokens, out_grad, head_grad, master_w, moment_m, moment_v, learn_rate, clip_scale):
        rows = master_w.shape[0]
        part = class_sums(tokens, out_grad, n_tp, rows)
        embed_grad = reduce_and_place(part, n_x, n_tp, rows)
        return adafactor_update(embed_grad, head_grad, master_w, moment_m, moment_v, learn_rate, clip_scale)

    return jax.shard_map(local_step, mesh=mesh, in_specs=(row_spec, act_spec, table_spec, table_spec, table_spec, table_spec, P(), P()), out_specs=(table_spec, table_spec, table_spec, table_spec), check_vma=False)
```

```python
import functools

import jax
import jax.numpy as jnp
import numpy as np
from jax import lax
from jax.experimental import pallas as pl
from jax.experimental.pallas import tpu as pltpu
from jax.sharding import PartitionSpec as P

OPT_STEP = 20
LANES = 128
TILE = 256
GROUP = 16
CORES = 2
PIECES = 2
CHUNKS = 8
CAPACITY = 272
SLOT_BITS = 9
FIRST, DIRECT, SECOND = 4, 2, 1
MESH = pl.DeviceIdType.MESH


def bits(power):
    return int(power).bit_length() - 1


def layout(rows, n_tp):
    sub = rows // n_tp
    span = pl.next_power_of_2(pl.cdiv(sub, CHUNKS))
    return sub, span, span * n_tp, span * n_tp * CHUNKS


def adafactor_update(embed_grad, head_grad, master_w, moment_m, moment_v, learn_rate, clip_scale):
    beta_two = 1.0 - OPT_STEP ** -0.8
    grad_full = clip_scale * (embed_grad + head_grad)
    new_v = beta_two * moment_v + (1.0 - beta_two) * (grad_full * grad_full + 1e-30)
    new_m = 0.9 * moment_m + 0.1 * (grad_full / jnp.sqrt(new_v))
    new_w = master_w - learn_rate * new_m - learn_rate * learn_rate * master_w
    return new_w, new_m, new_v, new_w.astype(jnp.bfloat16)


def count_of(key_ref, base, seq_len, pad):
    count = jnp.int32(0)
    half = seq_len // 2
    while half:
        count = jnp.where(key_ref[base + count + half - 1] & pad == 0, count + half, count)
        half //= 2
    return jnp.where(key_ref[base + count] & pad == 0, count + 1, count)


def tile_sums(rows, n_tp, key, tok, x_ref, onehot, sums):
    sub, span, chunk, size = layout(rows, n_tp)
    seq_len, width = x_ref.shape[1:]
    sum_pitch = sums.shape[0] // (width // LANES)
    place = key >> SLOT_BITS & (size - 1)
    row = ((place & (chunk - 1)) >> bits(span)) * sub + (place & (span - 1)) * CHUNKS + (place >> bits(chunk))
    ids = jnp.where(key & size << SLOT_BITS == 0, row * n_tp + lax.axis_index("tp"), -1)
    eye = lax.broadcasted_iota(jnp.int32, (TILE, TILE), 0) == lax.broadcasted_iota(jnp.int32, (TILE, TILE), 1)
    col = jnp.sum(jnp.where(eye, ids.astype(jnp.float32), 0.0), axis=1, keepdims=True).astype(jnp.int32)
    step = 512
    for j in range(0, seq_len, step):
        hit = col == tok[:, j : j + step]
        onehot[:, j : j + step] = jnp.where(hit, 1.0, 0.0).astype(jnp.bfloat16)
    for c in range(0, width // LANES, 2):
        part = jnp.dot(onehot[...], x_ref[0, :, c * LANES : (c + 2) * LANES], preferred_element_type=jnp.float32)
        sums[c * sum_pitch : c * sum_pitch + TILE, :] = part[:, :LANES]
        sums[(c + 1) * sum_pitch : (c + 1) * sum_pitch + TILE, :] = part[:, LANES:]


def clear(acc):
    step = 8 * 28

    def zero(i, carry):
        acc[pl.ds(pl.multiple_of(i * step, 8), step), :] = jnp.zeros((step, LANES), jnp.float32)
        return carry

    lax.fori_loop(0, acc.shape[0] // step, zero, 0)
    rest = acc.shape[0] % step
    if rest:
        acc[acc.shape[0] - rest :, :] = jnp.zeros((rest, LANES), jnp.float32)


def add_rows(acc, sums, g, addresses):
    blocks = 8
    pitch, sum_pitch = acc.shape[0] // blocks, sums.shape[0] // blocks
    old = [acc[pl.ds(a, blocks, stride=pitch), :] for a in addresses]
    new = [o + sums[pl.ds(g * GROUP + i, blocks, stride=sum_pitch), :] for i, o in enumerate(old)]
    for a, v in zip(addresses, new):
        acc[pl.ds(a, blocks, stride=pitch), :] = v


def scatter_kernel(rows, n_tp, key_ref, tok_ref, list_ref, x_ref, out_ref, acc, onehot, sums, sem):
    b = pl.program_id(0)
    seq_len, width = x_ref.shape[1:]
    blocks = width // LANES
    pitch = acc.shape[0] // blocks
    sub, span, chunk, size = layout(rows, n_tp)
    base = b * seq_len

    @pl.when(b == 0)
    def _():
        clear(acc)

    count = count_of(key_ref, base, seq_len, size << SLOT_BITS)
    tok = tok_ref[pl.ds(b, 1), :]

    def tile(k, carry):
        tile_sums(rows, n_tp, list_ref[0, pl.ds(k, 1), :], tok, x_ref, onehot, sums)

        def group(g, carry):
            first = base + k * TILE + g * GROUP
            addresses = []
            for i in range(GROUP):
                place = key_ref[first + i] >> SLOT_BITS & (2 * size - 1)
                row = ((place & (chunk - 1)) >> bits(span)) * sub + (place & (span - 1)) * CHUNKS + (place >> bits(chunk))
                addresses.append(jnp.where(place < size, row, rows))
            add_rows(acc, sums, g, addresses)
            return carry

        lax.fori_loop(0, (jnp.minimum(count - k * TILE, TILE) + GROUP - 1) // GROUP, group, 0)
        return carry

    lax.fori_loop(0, (count + TILE - 1) // TILE, tile, 0)

    @pl.when(b == pl.num_programs(0) - 1)
    def _():
        copies = [
            pltpu.make_async_copy(acc.at[pl.ds(c * pitch, rows), :], out_ref.at[c], sem.at[c]) for c in range(blocks)
        ]
        for copy in copies:
            copy.start()
        for copy in copies:
            copy.wait()


def class_sums(keys, tokens, out_grad, n_tp, rows):
    n_seq, seq_len, width = out_grad.shape
    blocks = width // LANES
    return pl.pallas_call(
        functools.partial(scatter_kernel, rows, n_tp),
        out_shape=jax.ShapeDtypeStruct((blocks, rows, LANES), jnp.float32),
        grid_spec=pltpu.PrefetchScalarGridSpec(
            num_scalar_prefetch=1,
            grid=(n_seq,),
            in_specs=[
                pl.BlockSpec((n_seq, seq_len), lambda b, *_: (0, 0)),
                pl.BlockSpec((1, seq_len // TILE, TILE), lambda b, *_: (b, 0, 0)),
                pl.BlockSpec((1, seq_len, width), lambda b, *_: (b, 0, 0)),
            ],
            out_specs=pl.BlockSpec(memory_space=pl.ANY),
            scratch_shapes=[
                pltpu.VMEM((blocks * (rows + 8), LANES), jnp.float32),
                pltpu.VMEM((TILE, seq_len), jnp.bfloat16),
                pltpu.VMEM((blocks * (TILE + 8), LANES), jnp.float32),
                pltpu.SemaphoreType.DMA((blocks,)),
            ],
        ),
        compiler_params=pltpu.CompilerParams(vmem_limit_bytes=60 * 1024 * 1024, dimension_semantics=("arbitrary",)),
        name="class_sums",
    )(keys, tokens, keys.reshape(n_seq, seq_len // TILE, TILE), out_grad)


def split_rows(rows, pieces):
    tiles = rows // 8
    sizes = [tiles // (2 * pieces) + (i < tiles % (2 * pieces)) for i in range(2 * pieces)]
    starts = [8 * sum(sizes[:i]) for i in range(2 * pieces)]
    spans = [(s, 8 * n) for s, n in zip(starts, sizes)]
    return spans[0::2], spans[1::2]


def exchange_kernel(n_x, n_tp, spans, part, out, own, sib, rec, got, load_sem, sib_sem, ring_sem, y_sem):
    pos = lax.axis_index("fsdp")
    me_y = lax.axis_index("tp")
    core = lax.rem(pos, CORES)
    me_x = pos // CORES
    other = 1 - core

    def at_x(x):
        return {"fsdp": lax.rem(x + n_x, n_x) * CORES + core}

    def at_y(d):
        return {"tp": lax.rem(me_y + d, n_tp)}

    sibling = {"fsdp": me_x * CORES + other}
    sides = [at_x(me_x + 1), at_x(me_x + n_x - 1)]

    barrier = pltpu.get_barrier_semaphore()
    peers = [sibling] + sides + [at_y(d) for d in range(1, n_tp)]
    for peer in peers:
        pl.semaphore_signal(barrier, inc=1, device_id=peer, device_id_type=MESH)
    pl.semaphore_wait(barrier, len(peers))

    def load(p, d):
        s, n = spans[d][p]
        return pltpu.make_async_copy(part.at[:, core, :, pl.ds(s, n), :], own.at[:, :, pl.ds(s, n), :], load_sem.at[d, p])

    def to_sibling(p, d):
        s, n = spans[d][p]
        return pltpu.make_async_remote_copy(
            src_ref=part.at[:, other, :, pl.ds(s, n), :],
            dst_ref=sib.at[:, :, pl.ds(s, n), :],
            send_sem=sib_sem.at[0, d, p],
            recv_sem=sib_sem.at[1, d, p],
            device_id=sibling,
            device_id_type=MESH,
        )

    def owner(d, step):
        return lax.rem(me_x + n_x - step, n_x) if d == 0 else lax.rem(me_x + step, n_x)

    def hop(p, d, step):
        s, n = spans[d][p]
        return pltpu.make_async_remote_copy(
            src_ref=own.at[owner(d, step), :, pl.ds(s, n), :],
            dst_ref=rec.at[step - 1, :, pl.ds(s, n), :],
            send_sem=ring_sem.at[0, d, step - 1, p],
            recv_sem=ring_sem.at[1, d, step - 1, p],
            device_id=sides[d],
            device_id_type=MESH,
        )

    def to_row(p, d, k):
        s, n = spans[d][p]
        return pltpu.make_async_remote_copy(
            src_ref=own.at[me_x, lax.rem(me_y + k, n_tp), pl.ds(s, n), :],
            dst_ref=got.at[k - 1, pl.ds(s, n), :],
            send_sem=y_sem.at[0, d, k - 1, p],
            recv_sem=y_sem.at[1, d, k - 1, p],
            device_id=at_y(k),
            device_id_type=MESH,
        )

    def add(p, d, step):
        s, n = spans[d][p]
        x = owner(d, step)
        for y in range(n_tp):
            total = own[x, y, pl.ds(s, n), :] + sib[x, y, pl.ds(s, n), :]
            if step > 1:
                total = total + rec[step - 2, y, pl.ds(s, n), :]
            own[x, y, pl.ds(s, n), :] = total

    pieces = len(spans[0])
    for p in range(pieces):
        for d in range(2):
            load(p, d).start()
            to_sibling(p, d).start()

    for t in range(pieces + n_x - 1):
        for step in range(1, n_x + 1):
            p = t - step + 1
            if not 0 <= p < pieces:
                continue
            for d in range(2):
                if step == 1:
                    load(p, d).wait()
                    to_sibling(p, d).wait_recv()
                else:
                    hop(p, d, step - 1).wait_recv()
                add(p, d, step)
                if step < n_x:
                    hop(p, d, step).start()
                else:
                    for k in range(1, n_tp):
                        to_row(p, d, k).start()

    for p in range(pieces):
        for d in range(2):
            s, n = spans[d][p]
            out[pl.ds(s * n_tp + me_y, n, stride=n_tp), :] = own[me_x, me_y, pl.ds(s, n), :]
            for k in range(1, n_tp):
                to_row(p, d, k).wait_recv()
                source = lax.rem(me_y + n_tp - k, n_tp)
                out[pl.ds(s * n_tp + source, n, stride=n_tp), :] = got[k - 1, pl.ds(s, n), :]

    for p in range(pieces):
        for d in range(2):
            to_sibling(p, d).wait_send()
            for step in range(1, n_x):
                hop(p, d, step).wait_send()
            for k in range(1, n_tp):
                to_row(p, d, k).wait_send()


def reduce_and_place(part, n_x, n_tp, rows):
    sub = rows // n_tp
    spans = split_rows(sub, PIECES)
    full = (n_x, n_tp, sub, LANES)
    return pl.pallas_call(
        functools.partial(exchange_kernel, n_x, n_tp, spans),
        out_shape=jax.ShapeDtypeStruct((rows, LANES), jnp.float32),
        in_specs=[pl.BlockSpec(memory_space=pl.ANY)],
        out_specs=pl.BlockSpec(memory_space=pltpu.VMEM),
        scratch_shapes=[
            pltpu.VMEM(full, jnp.float32),
            pltpu.VMEM(full, jnp.float32),
            pltpu.VMEM((n_x - 1, n_tp, sub, LANES), jnp.float32),
            pltpu.VMEM((n_tp - 1, sub, LANES), jnp.float32),
            pltpu.SemaphoreType.DMA((2, PIECES)),
            pltpu.SemaphoreType.DMA((2, 2, PIECES)),
            pltpu.SemaphoreType.DMA((2, 2, n_x - 1, PIECES)),
            pltpu.SemaphoreType.DMA((2, 2, n_tp - 1, PIECES)),
        ],
        compiler_params=pltpu.CompilerParams(
            collective_id=0, has_side_effects=True, vmem_limit_bytes=62 * 1024 * 1024
        ),
        name="reduce_and_place",
    )(part.reshape(n_x, CORES, n_tp, sub, LANES))


def slot_kernel(size, chunk, n_seq, s_ref, key_ref, over_ref):
    s = s_ref[...]
    height, absent = s.shape[0], CAPACITY - 1
    row = lax.broadcasted_iota(jnp.int32, s.shape, 0)
    lane = lax.broadcasted_iota(jnp.int32, s.shape, 1)
    turned = pltpu.roll(s, 1, 1)
    previous = jnp.where(lane == 0, pltpu.roll(turned, 1, 0), turned)
    previous = jnp.where((lane == 0) & (row == 0), -1, previous)
    place = s >> bits(n_seq)
    fresh = ((place != previous >> bits(n_seq)) & (place < size)).astype(jnp.float32)
    upto = lax.broadcasted_iota(jnp.int32, (LANES, LANES), 0) <= lax.broadcasted_iota(jnp.int32, (LANES, LANES), 1)
    inner = jnp.dot(fresh.astype(jnp.bfloat16), upto.astype(jnp.float32).astype(jnp.bfloat16), preferred_element_type=jnp.float32)
    total = jnp.broadcast_to(inner[:, LANES - 1 :], s.shape).astype(jnp.bfloat16)
    above = lax.broadcasted_iota(jnp.int32, (height, height), 1) < lax.broadcasted_iota(jnp.int32, (height, height), 0)
    outer = jnp.dot(above.astype(jnp.float32).astype(jnp.bfloat16), total, preferred_element_type=jnp.float32)
    rank = (inner + outer).astype(jnp.int32) - 1
    part = place >> bits(chunk)
    ends = [jnp.sum(jnp.where(part <= q, fresh, 0.0)).astype(jnp.int32) for q in range(CHUNKS)]
    start = jnp.zeros_like(s)
    over = (ends[0] > absent).astype(jnp.int32)
    for q in range(1, CHUNKS):
        start = jnp.where(part == q, ends[q - 1], start)
        over = jnp.maximum(over, (ends[q] - ends[q - 1] > absent).astype(jnp.int32))
    slot = jnp.minimum(rank - start, absent)
    padding = (s == previous) | (place >= size)
    low = jnp.where(padding, size << SLOT_BITS, (place << SLOT_BITS) + slot)
    key_ref[...] = (s & (n_seq - 1)) * (2 * size << SLOT_BITS) + low
    over_ref[0] = over


def sorted_keys(tokens, n_tp, rows):
    n_seq, seq_len = tokens.shape
    sub, span, chunk, size = layout(rows, n_tp)
    row = tokens // n_tp
    inner = row % sub
    place = inner % CHUNKS * chunk + row // sub * span + inner // CHUNKS
    place = jnp.where(tokens % n_tp == lax.axis_index("tp"), place, size)
    key = lax.sort((place * n_seq + lax.broadcasted_iota(jnp.int32, tokens.shape, 0)).reshape(-1))
    key, over = pl.pallas_call(
        functools.partial(slot_kernel, size, chunk, n_seq),
        out_shape=(jax.ShapeDtypeStruct((key.shape[0] // LANES, LANES), jnp.int32), jax.ShapeDtypeStruct((1,), jnp.int32)),
        out_specs=(pl.BlockSpec(memory_space=pltpu.VMEM), pl.BlockSpec(memory_space=pltpu.SMEM)),
        name="slots",
    )(key.reshape(-1, LANES))
    return lax.sort(key.reshape(-1)), over


def compact_kernel(rows, n_tp, key_ref, over_ref, tok_ref, list_ref, x_ref, empty_ref, out_ref, table_ref, acc, onehot, sums, table, sem):
    b = pl.program_id(0)
    seq_len, width = x_ref.shape[1:]
    blocks = width // LANES
    pitch = acc.shape[0] // blocks
    sub, span, chunk, size = layout(rows, n_tp)
    base = b * seq_len

    @pl.when(b == 0)
    def _():
        fill = pltpu.make_async_copy(empty_ref, table, sem.at[0])
        fill.start()
        clear(acc)
        fill.wait()

    count = count_of(key_ref, base, seq_len, size << SLOT_BITS)
    tok = tok_ref[pl.ds(b, 1), :]

    def tile(k, carry):
        tile_sums(rows, n_tp, list_ref[0, pl.ds(k, 1), :], tok, x_ref, onehot, sums)

        def group(g, carry):
            first = base + k * TILE + g * GROUP
            addresses = []
            for i in range(GROUP):
                key = key_ref[first + i]
                slot = key & ((1 << SLOT_BITS) - 1)
                place = key >> SLOT_BITS & (2 * size - 1)
                table[place] = slot
                addresses.append((place >> bits(chunk)) * CAPACITY + slot)
            add_rows(acc, sums, g, addresses)
            return carry

        lax.fori_loop(0, (jnp.minimum(count - k * TILE, TILE) + GROUP - 1) // GROUP, group, 0)
        return carry

    lax.fori_loop(0, (count + TILE - 1) // TILE, tile, 0)

    @pl.when(b == pl.num_programs(0) - 1)
    def _():
        table[span - 1] = over_ref[0]
        copies = [
            pltpu.make_async_copy(acc.at[pl.ds(c * pitch, CHUNKS * CAPACITY), :], out_ref.at[c], sem.at[c + 1])
            for c in range(blocks)
        ]
        copies.append(pltpu.make_async_copy(table.at[pl.ds(0, size)], table_ref, sem.at[0]))
        for copy in copies:
            copy.start()
        for copy in copies:
            copy.wait()


def compact_sums(keys, over, tokens, out_grad, n_tp, rows):
    n_seq, seq_len, width = out_grad.shape
    blocks = width // LANES
    _, span, chunk, size = layout(rows, n_tp)
    empty = np.full((size + chunk,), CAPACITY - 1, np.int32)
    empty[size:] = 0
    empty[span - 1] = 0
    return pl.pallas_call(
        functools.partial(compact_kernel, rows, n_tp),
        out_shape=(
            jax.ShapeDtypeStruct((blocks, CHUNKS * CAPACITY, LANES), jnp.float32),
            jax.ShapeDtypeStruct((size,), jnp.int32),
        ),
        grid_spec=pltpu.PrefetchScalarGridSpec(
            num_scalar_prefetch=2,
            grid=(n_seq,),
            in_specs=[
                pl.BlockSpec((n_seq, seq_len), lambda b, *_: (0, 0)),
                pl.BlockSpec((1, seq_len // TILE, TILE), lambda b, *_: (b, 0, 0)),
                pl.BlockSpec((1, seq_len, width), lambda b, *_: (b, 0, 0)),
                pl.BlockSpec(memory_space=pl.ANY),
            ],
            out_specs=(pl.BlockSpec(memory_space=pl.ANY), pl.BlockSpec(memory_space=pl.ANY)),
            scratch_shapes=[
                pltpu.VMEM((blocks * (CHUNKS * CAPACITY + 8), LANES), jnp.float32),
                pltpu.VMEM((TILE, seq_len), jnp.bfloat16),
                pltpu.VMEM((blocks * (TILE + 8), LANES), jnp.float32),
                pltpu.SMEM((size + chunk,), jnp.int32),
                pltpu.SemaphoreType.DMA((blocks + 1,)),
            ],
        ),
        compiler_params=pltpu.CompilerParams(vmem_limit_bytes=40 * 1024 * 1024, dimension_semantics=("arbitrary",)),
        name="compact_sums",
    )(keys, over, tokens, keys.reshape(n_seq, seq_len // TILE, TILE), out_grad, jnp.asarray(empty))


def star_kernel(rows, n_x, n_tp, comp, table, out, tables, *scratch):
    rec = scratch[:CHUNKS]
    transit, dense, got, lookup, table_sem, direct_sem, rec_sem, transit_sem, forward_sem, y_sem = scratch[CHUNKS:]
    sub, span, chunk, size = layout(rows, n_tp)
    n_f = n_x * CORES
    pos = lax.axis_index("fsdp")
    me_y = lax.axis_index("tp")
    core = lax.rem(pos, CORES)
    me_x = pos // CORES

    def at(dx, c):
        return lax.rem(me_x + n_x + dx, n_x) * CORES + c

    near = [at(0, 1 - core), at(1, 0), at(1, 1), at(-1, 0), at(-1, 1)]
    others = [lax.rem(pos + k, n_f) for k in range(1, n_f)]

    def at_y(d):
        return {"tp": lax.rem(me_y + d, n_tp)}

    barrier = pltpu.get_barrier_semaphore()
    peers = [{"fsdp": f} for f in others] + [at_y(d) for d in range(1, n_tp)]
    for peer in peers:
        pl.semaphore_signal(barrier, inc=1, device_id=peer, device_id_type=MESH)
    pl.semaphore_wait(barrier, len(peers))

    def remote(src, dst, send, recv, device):
        return pltpu.make_async_remote_copy(
            src_ref=src, dst_ref=dst, send_sem=send, recv_sem=recv, device_id=device, device_id_type=MESH
        )

    def rows_of(dest, q):
        return comp.at[dest, pl.ds(q * CAPACITY, CAPACITY), :]

    def direct(q, j):
        return remote(rows_of(near[j], q), rec[q].at[pos], direct_sem.at[q, j], rec_sem.at[q, pos], {"fsdp": near[j]})

    def stay(q):
        return pltpu.make_async_copy(rows_of(pos, q), rec[q].at[pos], rec_sem.at[q, pos])

    def turn(q):
        return 1 if q % 2 == 0 else -1

    def first_leg(q, c):
        return remote(
            rows_of(at(2, c), q), transit.at[q, c], transit_sem.at[0, q, c], transit_sem.at[1, q, c], {"fsdp": at(turn(q), core)}
        )

    def second_leg(q, c):
        origin = at(-turn(q), core)
        return remote(
            transit.at[q, c], rec[q].at[origin], forward_sem.at[q, c], rec_sem.at[q, origin], {"fsdp": at(turn(q), c)}
        )

    def arrival(q, f):
        return remote(rec[q].at[f], rec[q].at[f], direct_sem.at[q, 0], rec_sem.at[q, f], {"fsdp": near[0]})

    def table_to(k):
        mine = tables.at[pl.ds(pos * size, size)]
        return remote(table, mine, table_sem.at[0, k], table_sem.at[1, pos], {"fsdp": others[k]})

    def table_from(k):
        theirs = tables.at[pl.ds(others[k] * size, size)]
        return remote(table, theirs, table_sem.at[0, k], table_sem.at[1, others[k]], {"fsdp": others[k]})

    def to_row(q, k):
        return remote(
            dense.at[q, pl.ds(lax.rem(me_y + k, n_tp) * span, span), :], got.at[q, k - 1], y_sem.at[0, q, k - 1], y_sem.at[1, q, k - 1], at_y(k)
        )

    def start_first(q):
        if q < CHUNKS:
            for c in range(CORES):
                first_leg(q, c).start()

    def start_direct(q):
        if q < CHUNKS:
            for j in range(len(near)):
                direct(q, j).start()
            stay(q).start()

    def start_second(q):
        if q < CHUNKS:
            for c in range(CORES):
                first_leg(q, c).wait_recv()
                second_leg(q, c).start()

    for q in range(max(FIRST, DIRECT)):
        if q < FIRST:
            start_first(q)
        if q < DIRECT:
            start_direct(q)
        if q == 0:
            for k in range(n_f - 1):
                table_to(k).start()
    own_table = pltpu.make_async_copy(table, lookup.at[pl.ds(pos * size, size)], table_sem.at[2, pos])
    own_table.start()
    for k in range(n_f - 1):
        table_from(k).wait_recv()
        f = others[k]
        pltpu.make_async_copy(tables.at[pl.ds(f * size, size)], lookup.at[pl.ds(f * size, size)], table_sem.at[2, f]).start()
    own_table.wait()
    for k in range(n_f - 1):
        f = others[k]
        pltpu.make_async_copy(tables.at[pl.ds(f * size, size)], lookup.at[pl.ds(f * size, size)], table_sem.at[2, f]).wait()

    def expand(q, y, n):
        def eight(g, carry):
            for i in range(8):
                entry = q * chunk + y * span + g * 8 + i
                total = rec[q][0, pl.ds(lookup[entry], 1), :]
                for f in range(1, n_f):
                    total = total + rec[q][f, pl.ds(lookup[f * size + entry], 1), :]
                dense[q, pl.ds(y * span + g * 8 + i, 1), :] = total
            return carry

        lax.fori_loop(0, n * span // 8, eight, 0)

    def mark(q, y):
        over = lookup[span - 1]
        for f in range(1, n_f):
            over = over + lookup[f * size + span - 1]
        dense[q, y * span + span - 1 : y * span + span, :] = jnp.full((1, LANES), over.astype(jnp.float32))

    def place(q):
        out[pl.ds(q * n_tp + me_y, span, stride=CHUNKS * n_tp), :] = dense[q, pl.ds(me_y * span, span), :]
        for k in range(1, n_tp):
            to_row(q, k).wait_recv()
            source = lax.rem(me_y + n_tp - k, n_tp)
            out[pl.ds(q * n_tp + source, span, stride=CHUNKS * n_tp), :] = got[q, k - 1]

    for t in range(CHUNKS + 1):
        if t < CHUNKS:
            for q in range(SECOND + 1) if t == 0 else [t + SECOND]:
                start_second(q)
            start_first(t + FIRST)
            start_direct(t + DIRECT)
        if t > 0:
            q = t - 1
            stay(q).wait()
            for f in others:
                arrival(q, f).wait_recv()
            if t < CHUNKS:
                expand(q, 0, n_tp)
                if q == 0:
                    for y in range(n_tp):
                        mark(q, y)
                for k in range(1, n_tp):
                    to_row(q, k).start()
            else:
                for k in [n_tp // 2] + [k for k in range(1, n_tp) if k != n_tp // 2]:
                    expand(q, lax.rem(me_y + k, n_tp), 1)
                    to_row(q, k).start()
                expand(q, me_y, 1)
            if q > 1:
                place(q - 2)
    for q in range(CHUNKS - 2, CHUNKS):
        place(q)

    for k in range(n_f - 1):
        table_to(k).wait_send()
    for q in range(CHUNKS):
        for j in range(len(near)):
            direct(q, j).wait_send()
        for c in range(CORES):
            first_leg(q, c).wait_send()
            second_leg(q, c).wait_send()
        for k in range(1, n_tp):
            to_row(q, k).wait_send()


def exchange_compact(comp, table, n_x, n_tp, rows):
    _, span, chunk, size = layout(rows, n_tp)
    n_f = n_x * CORES
    dma = pltpu.SemaphoreType.DMA
    out, _ = pl.pallas_call(
        functools.partial(star_kernel, rows, n_x, n_tp),
        out_shape=(
            jax.ShapeDtypeStruct((CHUNKS * chunk, LANES), jnp.float32),
            jax.ShapeDtypeStruct((n_f * size,), jnp.int32),
        ),
        in_specs=[pl.BlockSpec(memory_space=pl.ANY)] * 2,
        out_specs=(pl.BlockSpec(memory_space=pltpu.VMEM), pl.BlockSpec(memory_space=pl.ANY)),
        scratch_shapes=[pltpu.VMEM((n_f, CAPACITY, LANES), jnp.float32) for _ in range(CHUNKS)]
        + [
            pltpu.VMEM((CHUNKS, CORES, CAPACITY, LANES), jnp.float32),
            pltpu.VMEM((CHUNKS, chunk, LANES), jnp.float32),
            pltpu.VMEM((CHUNKS, n_tp - 1, span, LANES), jnp.float32),
            pltpu.SMEM((n_f * size,), jnp.int32),
            dma((3, n_f)),
            dma((CHUNKS, 5)),
            dma((CHUNKS, n_f)),
            dma((2, CHUNKS, CORES)),
            dma((CHUNKS, CORES)),
            dma((2, CHUNKS, n_tp - 1)),
        ],
        compiler_params=pltpu.CompilerParams(
            collective_id=1, has_side_effects=True, vmem_limit_bytes=40 * 1024 * 1024
        ),
        name="exchange_compact",
    )(comp, table)
    return out


def solution(mesh):
    row_spec = P(("dp", "fsdp"), None)
    act_spec = P(("dp", "fsdp"), None, None)
    table_spec = P(("dp", "tp"), "fsdp")
    n_tp = mesh.shape["tp"]
    n_x = mesh.shape["fsdp"] // CORES

    def local_step(tokens, out_grad, head_grad, master_w, moment_m, moment_v, learn_rate, clip_scale):
        rows = master_w.shape[0]
        state = (head_grad, master_w, moment_m, moment_v, learn_rate, clip_scale)
        keys, over = sorted_keys(tokens, n_tp, rows)
        comp, table = compact_sums(keys, over, tokens, out_grad, n_tp, rows)
        placed = exchange_compact(comp, table, n_x, n_tp, rows)
        _, span, _, _ = layout(rows, n_tp)
        first = (span - 1) * CHUNKS * n_tp

        def dense(placed):
            own_keys = keys + (placed[first, 0] < 0.0).astype(jnp.int32)
            part = class_sums(own_keys, tokens, out_grad, n_tp, rows)
            return jnp.pad(reduce_and_place(part, n_x, n_tp, rows), ((0, placed.shape[0] - rows), (0, 0)))

        placed = lax.while_loop(lambda g: jnp.sum(g[first : first + n_tp, 0]) > 0.0, dense, placed)
        return adafactor_update(placed[:rows], *state)

    return jax.shard_map(local_step, mesh=mesh, in_specs=(row_spec, act_spec, table_spec, table_spec, table_spec, table_spec, P(), P()), out_specs=(table_spec, table_spec, table_spec, table_spec), check_vma=False)
```
